32 devices in a mesh: rep: 1, ep: 16 (over z, y, x), sub: 2 (over core).
Axes of the slice: x: 2, y: 2, z: 4, core: 2. Of those that a mesh axis runs over, the one named last changes fastest.
Arguments:
- tokens: bfloat16 [256, 5120], P(('rep', 'ep'), 'sub'), may hold values from -6 to 6
- expert_ids: int32 [256, 1], P(('rep', 'ep')), may hold values from 0 to 1; in each aligned block of 16 rows (0 to 15, 16 to 31, ...) at most 16 rows name the same one
- router_score: float32 [256, 1], P(('rep', 'ep')), may hold values from -8 to 8
- expert_gate_up: bfloat16 [5120, 2, 8192], P('sub', None, 'ep'), may hold values from -0.078125 to 0.078125
- expert_down: bfloat16 [8192, 5120], P('ep', 'sub'), may hold values from -0.09375 to 0.09375
- shared_gate_up: bfloat16 [5120, 2, 8192], P('sub', None, 'ep'), may hold values from -0.078125 to 0.078125
- shared_down: bfloat16 [8192, 5120], P('ep', 'sub'), may hold values from -0.0625 to 0.0625
Outputs:
- mixed: bfloat16 [256, 5120], P(('rep', 'ep'), 'sub')
The draws below stay inside these ranges and needn't reach their ends.
Inputs may be any that keep to these rules, and one draw needn't show every extreme that they name: `expert_ids`: in the rows of one index of ep (aligned blocks of 16 rows) no expert is named more than 16 times, a bound that some block reaches.
All inputs are finite; a program needn't handle non-finite values.
Results may differ from the reference program's by a relative error of at most 0.017.
Values may be sent and summed in bfloat16 or wider, within the bound.
No kernel may reach another device: no remote copies, remote signals or barrier semaphores. Data moves between devices by JAX's collectives and lax.ppermute only.
A program may use at most 64 MiB of HBM per device.

```python
import math
import jax
import jax.numpy as jnp
import numpy as np
from jax import lax

D = 5120
FF = 4096
FF_SH = 8192
EXP_ROWS = 8
TOK_ROW = 16
EXPERTS = 2
TOKENS = 256
CAP = 16
N_EP = 16


def levels(own_key, extent, shards, smallest, high):
    loudness = 1.0
    for axis_at, blocks in shards:
        heights = jax.random.uniform(jax.random.fold_in(jax.random.fold_in(own_key, 6), axis_at), (blocks,), jnp.float32, smallest / len(shards), high / len(shards))
        loudness = loudness * jnp.repeat(jnp.exp(heights), extent[axis_at] // blocks).reshape((-1,) + (1,) * (len(extent) - 1 - axis_at))
    return loudness


def routed_block(key, own, number, rows, count, top, reach, slope):
    order = jax.random.permutation(key, count)
    packed, common = load_shares(count, rows * top, reach, slope, True), load_shares(count, rows * top, reach, slope, False)
    places = jnp.arange(count)

    def named(lengths, turn):
        used = int((lengths > 0).sum())
        fixed = max(1, used // 4)
        moved = fixed + (places - fixed + turn * (used - fixed)) % max(1, count - fixed)
        return jnp.zeros((count,), jnp.int32).at[order[jnp.where(places < fixed, places, moved)]].set(jnp.asarray(lengths, jnp.int32))

    lengths = jnp.where(number % 4 == 0, named(packed, number // 4), named(common, number - number // 4 - 1))
    mixed = jax.random.permutation(jax.random.fold_in(own, 3), count)
    source_of, sink = mixed[0:count // 2 * 2:2], mixed[1:count // 2 * 2:2]
    room = jnp.minimum(lengths[source_of] - 1, reach - lengths[sink]) // 2
    room = jnp.where((source_of == order[0]) | (sink == order[0]) | (lengths[sink] == 0), 0, jnp.maximum(room, 0))
    moved = jax.random.randint(jax.random.fold_in(own, 4), (count // 2,), 0, 1 << 20) % (room + 1)
    lengths = lengths.at[source_of].add(-moved).at[sink].add(moved)
    labels = jnp.searchsorted(jnp.cumsum(lengths), jnp.arange(rows * top), side="right").astype(jnp.int32)
    listing = labels.reshape(top, rows).T
    listing = listing[jax.random.permutation(jax.random.fold_in(own, 1), rows)]
    turn = jax.random.randint(jax.random.fold_in(own, 2), (rows, 1), 0, top)
    return jnp.take_along_axis(listing, (jnp.arange(top)[None, :] + turn) % top, axis=1)


def load_shares(number_of, total, limit, slope, full):
    weights = [(1 << 20) // math.isqrt(grade ** slope) + 1 for grade in range(1, number_of + 1)]
    largest = limit if full else min(limit, max(-(-total // number_of), total * weights[0] // sum(weights)))
    least = 1 if total - largest >= number_of - 1 else 0
    given, spare = [largest] + [least] * (number_of - 1), total - largest - least * (number_of - 1)
    while spare > 0:
        candidates = [i for i in range(1, number_of) if given[i] < largest] or [i for i in range(1, number_of) if given[i] < limit]
        pool, remaining = sum([weights[i] for i in candidates]), spare
        for i in candidates:
            addition = min(limit - given[i], max(1, remaining * weights[i] // pool), spare)
            given[i] = given[i] + addition
            spare = spare - addition
    return np.array(given)


def centred(own_key, shape, scale, most, shards=(), kind=jnp.bfloat16):
    array = jax.random.normal(own_key, shape, jnp.float32) * scale
    if len(shards) > 0:
        array = levels(own_key, shape, shards, -0.22, 0.18) * array
    return jnp.clip(array, min=-most, max=most).astype(kind)


def setup_inputs(seed: int = 0, part: int = 0) -> dict:
    key_of = jax.random.split(jax.random.key(seed), 8)
    own_keys = jax.random.split(jax.random.fold_in(key_of[7], part), 8)
    tokens = centred(own_keys[0], (TOKENS, D), 1.0, 6.0, ((0, 16), (1, 2)))
    expert_ids_keys = jax.random.split(jax.random.fold_in(own_keys[1], 1), TOKENS // TOK_ROW)
    expert_ids_turns = jax.random.permutation(jax.random.fold_in(own_keys[1], 3), TOKENS // TOK_ROW)
    expert_ids = jax.vmap(lambda own, number: routed_block(jax.random.fold_in(own_keys[1], 2), own, number, TOK_ROW, EXPERTS, 1, CAP, 2))(expert_ids_keys, expert_ids_turns).reshape((TOKENS, 1))
    router_score = centred(own_keys[2], (TOKENS, 1), 2.0, 8.0, ((0, 16),), jnp.float32)
    expert_gate_up = centred(key_of[3], (D, 2, EXPERTS * FF), D ** -0.5, 0.078125, ((0, 2), (2, 16)))
    expert_down = centred(key_of[4], (EXPERTS * FF, D), FF ** -0.5, 0.09375, ((0, 16), (1, 2)))
    shared_gate_up = centred(key_of[5], (D, 2, FF_SH), D ** -0.5, 0.078125, ((0, 2), (2, 16)))
    shared_down = centred(key_of[6], (FF_SH, D), FF_SH ** -0.5, 0.0625, ((0, 16), (1, 2)))
    return {"tokens": tokens, "expert_ids": expert_ids, "router_score": router_score, "expert_gate_up": expert_gate_up, "expert_down": expert_down, "shared_gate_up": shared_gate_up, "shared_down": shared_down}


def slot_ranks(token_ids, experts):
    onehot = (token_ids[..., None] == jnp.arange(experts, dtype=jnp.int32)).astype(jnp.int32)
    before = jnp.cumsum(onehot, axis=-2) - onehot
    return jnp.sum(before * onehot, axis=-1)


def reference(tokens, expert_ids, router_score, expert_gate_up, expert_down, shared_gate_up, shared_down):
    token_ids = expert_ids[:, 0]
    position = slot_ranks(token_ids.reshape(N_EP, TOK_ROW), EXPERTS).reshape(-1)
    row_index = jnp.arange(TOKENS, dtype=jnp.int32) // TOK_ROW
    slot_index = (row_index * CAP + position).astype(jnp.int32)
    total_slots = N_EP * CAP
    gate = jax.nn.sigmoid(router_score)
    weighted = (gate * tokens.astype(jnp.float32)).astype(jnp.bfloat16)
    block_width = FF // EXP_ROWS

    def add_expert(expert, carry):
        chosen = (token_ids == expert)[:, None] & (slot_index[:, None] == jnp.arange(total_slots, dtype=jnp.int32)[None, :])
        select = chosen.astype(jnp.bfloat16)
        slot_rows = lax.dot_general(select, weighted, (((0,), (0,)), ((), ())), preferred_element_type=jnp.float32).astype(jnp.bfloat16)
        start = (expert * FF).astype(jnp.int32)
        gate_cols = lax.dynamic_slice_in_dim(expert_gate_up, start, FF, 2).reshape(D, 2 * FF)
        gate_up = jnp.dot(slot_rows, gate_cols, preferred_element_type=jnp.float32).reshape(total_slots, 2, FF)
        hidden = (jax.nn.silu(gate_up[:, 0]) * gate_up[:, 1]).astype(jnp.bfloat16)
        hidden = hidden.reshape(total_slots, EXP_ROWS, block_width).astype(jnp.float32)
        down_rows = lax.dynamic_slice_in_dim(expert_down, start, FF, 0).reshape(EXP_ROWS, block_width, D).astype(jnp.float32)
        parts = jnp.einsum("skh,khd->ksd", hidden, down_rows).astype(jnp.bfloat16)
        summed = jnp.sum(parts.astype(jnp.float32), axis=0)
        return carry + jnp.dot(select.astype(jnp.float32), summed, precision=lax.Precision.HIGHEST)

    routed = lax.fori_loop(0, EXPERTS, add_expert, jnp.zeros((TOKENS, D), jnp.float32))
    shared_sum = jnp.dot(tokens, shared_gate_up.reshape(D, 2 * FF_SH), preferred_element_type=jnp.float32).reshape(TOKENS, 2, FF_SH)
    shared_hidden = (jax.nn.silu(shared_sum[:, 0]) * shared_sum[:, 1]).astype(jnp.bfloat16)
    shared = jnp.dot(shared_hidden, shared_down, preferred_element_type=jnp.float32)
    return (shared + routed).astype(jnp.bfloat16)
```

```python
import jax
import jax.numpy as jnp
from jax import lax
from jax.sharding import PartitionSpec as P

EXP_ROWS = 8
LANES = 128
F32 = jnp.float32
BF16 = jnp.bfloat16


def stage_list(size):
    stages = []
    stride = 1
    while stride < size:
        radix = 4 if size // stride % 4 == 0 else 2
        stages.append((stride, radix))
        stride *= radix
    return stages[::-1]


def swap(value, size, offset):
    return lax.ppermute(value, "ep", [(i, i ^ offset) for i in range(size)])


def gather_rows(block, size):
    offsets = [0]
    for stride, radix in stage_list(size):
        parts = [block] + [swap(block, size, k * stride) for k in range(1, radix)]
        offsets = [o ^ (k * stride) for k in range(radix) for o in offsets]
        block = jnp.concatenate(parts, axis=0)
    return block, offsets


def scatter_sum(partial, size):
    for stride, radix in stage_list(size)[::-1]:
        rows = partial.shape[0] // radix
        parts = [partial[k * rows : (k + 1) * rows] for k in range(radix)]
        moved = [swap(parts[k].astype(BF16), size, k * stride) for k in range(1, radix)]
        partial = parts[0].astype(F32)
        for value in moved:
            partial = partial + value.astype(F32)
    return partial


def sub_sum(value):
    pairs = [(0, 1), (1, 0)]
    return value + lax.ppermute(value.astype(BF16), "sub", pairs).astype(F32)


def local(
    tokens, expert_ids, router_score, expert_gate_up, expert_down, shared_gate_up, shared_down
):
    rows_here, half_width = tokens.shape
    size = lax.axis_size("ep")
    experts = size // EXP_ROWS
    capacity = min(rows_here, max(2, 3 * rows_here // experts))
    hidden_width = expert_down.shape[0]
    shared_width = shared_down.shape[0]

    gate = jax.nn.sigmoid(router_score)
    gate_high = gate.astype(BF16)
    gate_low = (gate - gate_high.astype(F32)).astype(BF16)
    extra = jnp.concatenate([expert_ids.astype(BF16), gate_high, gate_low], axis=1)
    extra = jnp.pad(extra, ((0, 0), (0, LANES - extra.shape[1])))
    packed = jnp.concatenate([tokens, extra], axis=1)
    packed, _ = gather_rows(packed, size)
    all_tokens = packed[:, :half_width]
    all_ids = packed[:, half_width].astype(jnp.int32)
    all_gates = packed[:, half_width + 1].astype(F32) + packed[:, half_width + 2].astype(F32)

    own_expert = lax.axis_index("ep") // EXP_ROWS
    chosen = all_ids == own_expert
    scale = jnp.where(chosen, all_gates, 0.0)

    shared_in = shared_gate_up.reshape(half_width, 2 * shared_width)
    routed_in = expert_gate_up.reshape(half_width, 2 * hidden_width)
    shared_sum = sub_sum(jnp.dot(all_tokens, shared_in, preferred_element_type=F32))
    shared_hidden = jax.nn.silu(shared_sum[:, :shared_width]) * shared_sum[:, shared_width:]

    select = None
    routed_rows = all_tokens
    if capacity < rows_here:
        picked = chosen.reshape(size, rows_here).astype(jnp.int32)
        position = jnp.cumsum(picked, axis=1) - picked
        block = lax.broadcasted_iota(jnp.int32, (size, rows_here), 0)
        slot = jnp.where(picked == 1, block * capacity + position, -1).reshape(-1)
        slots = lax.broadcasted_iota(jnp.int32, (size * capacity, size * rows_here), 0)
        select = (slots == slot[None, :]).astype(BF16)
        weighted = (all_gates[:, None] * all_tokens.astype(F32)).astype(BF16)
        routed_rows = jnp.dot(select, weighted, preferred_element_type=F32).astype(BF16)
    routed_sum = jnp.dot(routed_rows, routed_in, preferred_element_type=F32)
    routed_sum = sub_sum(routed_sum)
    if select is None:
        routed_sum = routed_sum * scale[:, None]
    routed_hidden = jax.nn.silu(routed_sum[:, :hidden_width]) * routed_sum[:, hidden_width:]

    partial = jnp.dot(shared_hidden.astype(BF16), shared_down, preferred_element_type=F32)
    routed = jnp.dot(routed_hidden.astype(BF16), expert_down, preferred_element_type=F32)
    if select is not None:
        routed = lax.dot_general(
            select, routed.astype(BF16), (((0,), (0,)), ((), ())), preferred_element_type=F32
        )
    return scatter_sum(partial + routed, size).astype(BF16)


def solution(mesh):
    placed = (
        P(("rep", "ep"), "sub"),
        P(("rep", "ep"), None),
        P(("rep", "ep"), None),
        P("sub", None, "ep"),
        P("ep", "sub"),
        P("sub", None, "ep"),
        P("ep", "sub"),
    )
    return jax.shard_map(
        local, mesh=mesh, in_specs=placed, out_specs=P(("rep", "ep"), "sub"), check_vma=False
    )
```

```python
import functools

import jax
import jax.numpy as jnp
from jax import lax
from jax.experimental import pallas as pl
from jax.experimental.pallas import tpu as pltpu
from jax.sharding import PartitionSpec as P


EXP_ROWS = 8
LANES = 128
F32 = jnp.float32
BF16 = jnp.bfloat16
VMEM = pl.BlockSpec(memory_space=pltpu.VMEM)
HBM = pl.BlockSpec(memory_space=pltpu.HBM)


def stage_list(size):
    stages = []
    stride = 1
    while stride < size:
        radix = 4 if size // stride % 4 == 0 else 2
        stages.append((stride, radix))
        stride *= radix
    return stages


def swap(value, size, offset):
    return lax.ppermute(value, "ep", [(i, i ^ offset) for i in range(size)])


def call(body, outs, ins, args, limit, scratch=(), flops=0):
    return pl.pallas_call(
        body,
        out_shape=outs,
        in_specs=ins,
        out_specs=jax.tree.map(lambda _: VMEM, outs),
        scratch_shapes=scratch,
        compiler_params=pltpu.CompilerParams(vmem_limit_bytes=limit << 20),
        cost_estimate=pl.CostEstimate(
            flops=flops, bytes_accessed=sum(a.size * a.dtype.itemsize for a in args), transcendentals=0
        ),
    )(*args)


def like(shape, dtype):
    return jax.ShapeDtypeStruct(shape, dtype)


def pack_kernel(tokens_ref, ids_ref, score_ref, out_ref):
    rows, width = tokens_ref.shape
    here = lax.broadcasted_iota(jnp.int32, (rows, rows), 0)
    there = lax.broadcasted_iota(jnp.int32, (rows, rows), 1)

    def column(row):
        return jnp.sum(jnp.where(here == there, row, 0.0), axis=1, keepdims=True)

    ids = column(ids_ref[...].astype(F32))
    gate = 1.0 / (1.0 + jnp.exp(-column(score_ref[...])))
    high = gate.astype(BF16).astype(F32)
    lane = lax.broadcasted_iota(jnp.int32, (rows, LANES), 1)
    extra = jnp.where(lane == 0, ids, jnp.where(lane == 1, high, gate - high))
    out_ref[:, :width] = tokens_ref[...]
    out_ref[:, width:] = extra.astype(BF16)


def pack(tokens, ids, score):
    rows, width = tokens.shape
    return call(
        pack_kernel,
        like((rows, width + LANES), BF16),
        [VMEM] * 3,
        (tokens, ids.reshape(1, rows), score.reshape(1, rows)),
        2,
    )


def join_kernel(*refs):
    *parts, out_ref = refs
    row = 0
    for part in parts:
        out_ref[row : row + part.shape[0]] = part[...]
        row += part.shape[0]


def join(parts):
    rows = sum(part.shape[0] for part in parts)
    return call(
        join_kernel, like((rows, parts[0].shape[1]), BF16), [VMEM] * len(parts), tuple(parts), 8
    )


def gather_rows(block, size):
    *far, (stride, radix) = stage_list(size)[::-1]
    rest = []
    for far_stride, far_radix in far:
        whole = join([block] + rest) if rest else block
        moved = {k: swap(whole, size, k * far_stride) for k in range(far_radix - 1, 0, -1)}
        rest += [moved[k] for k in range(1, far_radix)]
    near = {k: swap(block, size, k * stride) for k in range(radix - 1, 0, -1)}
    rest = join(rest)
    moved = {k: swap(rest, size, k * stride) for k in range(radix - 1, 0, -1)}
    parts = [block, rest]
    for k in range(1, radix):
        parts += [near[k], moved[k]]
    return parts


def scatter_sum(own, total, near, rest, size):
    rows = own.shape[0]
    (stride, radix), *far = stage_list(size)
    rest = {k: swap(rest[k], size, k * stride) for k in range(radix - 1, 0, -1)}
    near = {k: swap(near[k], size, k * stride) for k in range(radix - 1, 0, -1)}
    for k in range(1, radix):
        total = total + rest[k].astype(F32)
    pieces = [near[k] for k in range(1, radix)]
    for far_stride, far_radix in far:
        count = (total.shape[0] + rows) // far_radix
        send = total.astype(BF16)
        moved = {
            k: swap(send[k * count - rows : (k + 1) * count - rows], size, k * far_stride)
            for k in range(far_radix - 1, 0, -1)
        }
        total = total[: count - rows]
        for k in range(1, far_radix):
            pieces.append(moved[k][:rows])
            total = total + moved[k][rows:].astype(F32)
    for piece in pieces:
        own = own + piece.astype(F32)
    return own


def split_kernel(order_ref, stored_ref, out_ref, slots, sems, *, chunk):
    depth, _, width = stored_ref.shape
    half = order_ref.shape[0] // 2
    count = slots.shape[0]
    steps = depth // chunk

    def fetch(step, slot):
        source = stored_ref.at[pl.ds(pl.multiple_of(step * chunk, chunk), chunk)]
        return pltpu.make_async_copy(source, slots.at[slot], sems.at[slot])

    for step in range(count):
        fetch(step, step).start()

    def body(step, carry):
        slot = lax.rem(step, count)
        fetch(step, slot).wait()
        for part in range(chunk // half):
            pairs = slots[slot, pl.ds(part * half, half)].reshape(2 * half, width)
            apart = jnp.dot(order_ref[...], pairs, preferred_element_type=F32).astype(BF16)
            rows = pl.ds(pl.multiple_of(step * chunk + part * half, half), half)
            out_ref[rows, :width] = apart[:half]
            out_ref[rows, width:] = apart[half:]

        @pl.when(step + count < steps)
        def _():
            fetch(step + count, slot).start()

        return carry

    lax.fori_loop(0, steps, body, 0)


def split_pairs(stored, order):
    depth, _, width = stored.shape
    chunk = 256
    slots = min(5, depth // chunk)
    return call(
        functools.partial(split_kernel, chunk=chunk),
        like((depth, 2 * width), BF16),
        [VMEM, HBM],
        (order, stored),
        12,
        scratch=[pltpu.VMEM((slots, chunk, 2, width), BF16), pltpu.SemaphoreType.DMA((slots,))],
        flops=4 * 2 * LANES * depth * 2 * width,
    )


def gate_up_kernel(*refs, count, depth):
    parts, weight_ref, send_ref, own_ref = refs[:count], *refs[count : count + 3]
    rows = jnp.concatenate([part[:, :depth] for part in parts], axis=0)
    total = jnp.dot(rows, weight_ref[...], preferred_element_type=F32)
    own_ref[...] = total
    send_ref[...] = total.astype(BF16)
    for extra_ref in refs[count + 3 :]:
        extra_ref[...] = jnp.concatenate([part[:, depth:] for part in parts], axis=0)


def gate_up(parts, weight, extra=False):
    depth, width = weight.shape
    rows = sum(part.shape[0] for part in parts)
    outs = [like((rows, width), BF16), like((rows, width), F32)]
    if extra:
        outs.append(like((rows, LANES), BF16))
    return call(
        functools.partial(gate_up_kernel, count=len(parts), depth=depth),
        outs,
        [VMEM] * (len(parts) + 1),
        (*parts, weight),
        20 + rows * width // (1 << 17) * 2,
        flops=2 * rows * depth * width,
    )


def sub_swap(send):
    return lax.ppermute(send, "sub", [(0, 1), (1, 0)])


def hidden_of(own_ref, moved_ref, scale=None):
    total = own_ref[...] + moved_ref[...].astype(F32)
    if scale is not None:
        total = total * scale
    width = total.shape[1] // 2
    gate = total[:, :width]
    return (gate / (1.0 + jnp.exp(-gate)) * total[:, width:]).astype(BF16)


def shared_down_kernel(own_ref, moved_ref, weight_ref, out_ref):
    hidden = hidden_of(own_ref, moved_ref)
    out_ref[...] = jnp.dot(hidden, weight_ref[...], preferred_element_type=F32)


def routed_down_kernel(own_ref, moved_ref, extra_ref, base_ref, weight_ref, *outs, rows, radix):
    expert = (lax.axis_index("ep") // EXP_ROWS).astype(F32)
    ids = extra_ref[:, :1].astype(F32)
    gate = extra_ref[:, 1:2].astype(F32) + extra_ref[:, 2:3].astype(F32)
    hidden = hidden_of(own_ref, moved_ref, jnp.where(ids == expert, gate, 0.0))
    partial = base_ref[...] + jnp.dot(hidden, weight_ref[...], preferred_element_type=F32)
    count = partial.shape[0] // radix
    for k in range(radix):
        near_ref, rest_ref = outs[2 * k], outs[2 * k + 1]
        near_ref[...] = partial[k * count : k * count + rows].astype(near_ref.dtype)
        rest_ref[...] = partial[k * count + rows : (k + 1) * count].astype(rest_ref.dtype)


def dense_experts(parts, shared_in, routed_in, shared_down, expert_down, rows, size):
    send_s, own_s, extra = gate_up(parts, shared_in, extra=True)
    moved_s = sub_swap(send_s)
    send_r, own_r = gate_up(parts, routed_in)
    moved_r = sub_swap(send_r)
    total_rows, width = send_s.shape[0], shared_down.shape[1]
    base = call(
        shared_down_kernel,
        like((total_rows, width), F32),
        [VMEM] * 3,
        (own_s, moved_s, shared_down),
        16,
        flops=2 * total_rows * shared_down.size,
    )
    radix = stage_list(size)[0][1]
    count = total_rows // radix
    outs = []
    for k in range(radix):
        kind = F32 if k == 0 else BF16
        outs += [like((rows, width), kind), like((count - rows, width), kind)]
    pieces = call(
        functools.partial(routed_down_kernel, rows=rows, radix=radix),
        outs,
        [VMEM] * 5,
        (own_r, moved_r, extra, base, expert_down),
        20,
        flops=2 * total_rows * expert_down.size,
    )
    near = {k: pieces[2 * k] for k in range(1, radix)}
    rest = {k: pieces[2 * k + 1] for k in range(1, radix)}
    return scatter_sum(pieces[0], pieces[1], near, rest, size)


def slot_experts(
    parts, shared_in, routed_in, shared_down, expert_down, rows, size, capacity, own_expert
):
    half_width = shared_in.shape[0]
    packed = jnp.concatenate(parts, axis=0)
    all_tokens = packed[:, :half_width]
    extra = packed[:, half_width:]
    all_gates = extra[:, 1].astype(F32) + extra[:, 2].astype(F32)
    picked = (extra[:, 0].astype(jnp.int32) == own_expert).reshape(size, rows).astype(jnp.int32)
    position = jnp.cumsum(picked, axis=1) - picked
    block = lax.broadcasted_iota(jnp.int32, (size, rows), 0)
    slot = jnp.where(picked == 1, block * capacity + position, -1).reshape(-1)
    slots = lax.broadcasted_iota(jnp.int32, (size * capacity, size * rows), 0)
    select = (slots == slot[None, :]).astype(BF16)
    weighted = (all_gates[:, None] * all_tokens.astype(F32)).astype(BF16)
    slot_rows = jnp.dot(select, weighted, preferred_element_type=F32).astype(BF16)

    def hidden(x, weight):
        total = jnp.dot(x, weight, preferred_element_type=F32)
        total = total + sub_swap(total.astype(BF16)).astype(F32)
        width = total.shape[1] // 2
        return (jax.nn.silu(total[:, :width]) * total[:, width:]).astype(BF16)

    shared = jnp.dot(hidden(all_tokens, shared_in), shared_down, preferred_element_type=F32)
    routed = jnp.dot(hidden(slot_rows, routed_in), expert_down, preferred_element_type=F32)
    partial = shared + lax.dot_general(
        select, routed.astype(BF16), (((0,), (0,)), ((), ())), preferred_element_type=F32
    )
    radix = stage_list(size)[0][1]
    count = partial.shape[0] // radix
    send = partial.astype(BF16)
    near = {k: send[k * count : k * count + rows] for k in range(1, radix)}
    rest = {k: send[k * count + rows : (k + 1) * count] for k in range(1, radix)}
    return scatter_sum(partial[:rows], partial[rows:count], near, rest, size)


def local(
    tokens, expert_ids, router_score, expert_gate_up, expert_down, shared_gate_up, shared_down
):
    rows = tokens.shape[0]
    size = lax.axis_size("ep")
    experts = size // EXP_ROWS
    capacity = min(rows, max(2, 3 * rows // experts))

    parts = gather_rows(pack(tokens, expert_ids, router_score), size)
    row = lax.broadcasted_iota(jnp.int32, (2 * LANES, 2 * LANES), 0)
    column = lax.broadcasted_iota(jnp.int32, (2 * LANES, 2 * LANES), 1)
    order = (column == 2 * (row % LANES) + row // LANES).astype(BF16)
    shared_in = split_pairs(shared_gate_up, order)
    routed_in = split_pairs(expert_gate_up, order)
    operands = (parts, shared_in, routed_in, shared_down, expert_down, rows, size)
    if capacity == rows:
        mixed = dense_experts(*operands)
    else:
        mixed = slot_experts(*operands, capacity, lax.axis_index("ep") // EXP_ROWS)
    return mixed.astype(BF16)


def solution(mesh):
    placed = (
        P(("rep", "ep"), "sub"),
        P(("rep", "ep"), None),
        P(("rep", "ep"), None),
        P("sub", None, "ep"),
        P("ep", "sub"),
        P("sub", None, "ep"),
        P("ep", "sub"),
    )
    return jax.shard_map(
        local, mesh=mesh, in_specs=placed, out_specs=P(("rep", "ep"), "sub"), check_vma=False
    )
```

```python
import functools

import jax
import jax.numpy as jnp
from jax import lax
from jax.experimental import pallas as pl
from jax.experimental.pallas import tpu as pltpu
from jax.sharding import PartitionSpec as P


EXP_ROWS = 8
LANES = 128
F32 = jnp.float32
BF16 = jnp.bfloat16
VMEM = pl.BlockSpec(memory_space=pltpu.VMEM)
HBM = pl.BlockSpec(memory_space=pltpu.HBM)


def stage_list(size):
    stages = []
    stride = 1
    while stride < size:
        radix = 4 if size // stride % 4 == 0 else 2
        stages.append((stride, radix))
        stride *= radix
    return stages


def swap(value, size, offset):
    return lax.ppermute(value, "ep", [(i, i ^ offset) for i in range(size)])


def call(body, outs, ins, args, limit, scratch=(), flops=0):
    return pl.pallas_call(
        body,
        out_shape=outs,
        in_specs=ins,
        out_specs=jax.tree.map(lambda _: VMEM, outs),
        scratch_shapes=scratch,
        compiler_params=pltpu.CompilerParams(vmem_limit_bytes=limit << 20),
        cost_estimate=pl.CostEstimate(
            flops=flops,
            bytes_accessed=sum(a.size * a.dtype.itemsize for a in args),
            transcendentals=0,
        ),
    )(*args)


def like(shape, dtype):
    return jax.ShapeDtypeStruct(shape, dtype)


def pack_kernel(tokens_hbm, ids_hbm, score_hbm, out_ref, ids_ref, score_ref, sems):
    rows, width = tokens_hbm.shape
    copies = [
        pltpu.make_async_copy(ids_hbm, ids_ref, sems.at[0]),
        pltpu.make_async_copy(score_hbm, score_ref, sems.at[1]),
        pltpu.make_async_copy(tokens_hbm, out_ref.at[:, pl.ds(0, width)], sems.at[2]),
    ]
    for copy in copies:
        copy.start()
    here = lax.broadcasted_iota(jnp.int32, (rows, rows), 0)
    there = lax.broadcasted_iota(jnp.int32, (rows, rows), 1)

    def column(row):
        return jnp.sum(jnp.where(here == there, row, 0.0), axis=1, keepdims=True)

    copies[0].wait()
    copies[1].wait()
    ids = column(ids_ref[...].astype(F32))
    gate = 1.0 / (1.0 + jnp.exp(-column(score_ref[...])))
    high = gate.astype(BF16).astype(F32)
    lane = lax.broadcasted_iota(jnp.int32, (rows, LANES), 1)
    extra = jnp.where(lane == 0, ids, jnp.where(lane == 1, high, gate - high))
    out_ref[:, width:] = extra.astype(BF16)
    copies[2].wait()


def pack(tokens, ids, score):
    rows, width = tokens.shape
    arrays = (tokens, ids.reshape(1, rows), score.reshape(1, rows))
    return call(
        pack_kernel,
        like((rows, width + LANES), BF16),
        [HBM] * 3,
        tuple(pltpu.with_memory_space_constraint(a, pltpu.HBM) for a in arrays),
        2,
        scratch=[
            pltpu.VMEM((1, rows), jnp.int32),
            pltpu.VMEM((1, rows), F32),
            pltpu.SemaphoreType.DMA((3,)),
        ],
    )


def join_kernel(*refs):
    *parts, out_ref = refs
    row = 0
    for part in parts:
        out_ref[row : row + part.shape[0]] = part[...]
        row += part.shape[0]


def join(parts):
    rows = sum(part.shape[0] for part in parts)
    return call(
        join_kernel, like((rows, parts[0].shape[1]), BF16), [VMEM] * len(parts), tuple(parts), 8
    )


def fold_kernel(*refs, offsets, spans):
    terms, outs = refs[: len(offsets)], refs[len(offsets) :]
    for (low, high), out_ref in zip(spans, outs):
        total = terms[0][offsets[0] + low : offsets[0] + high].astype(F32)
        for term, offset in zip(terms[1:], offsets[1:]):
            total = total + term[offset + low : offset + high].astype(F32)
        out_ref[...] = total.astype(out_ref.dtype)


def fold(terms, outs):
    width = terms[0][0].shape[1]
    arrays = tuple(term for term, _ in terms)
    return call(
        functools.partial(
            fold_kernel,
            offsets=tuple(offset for _, offset in terms),
            spans=tuple((low, high) for low, high, _ in outs),
        ),
        [like((high - low, width), kind) for low, high, kind in outs],
        [VMEM] * len(terms),
        arrays,
        sum(a.size * a.dtype.itemsize for a in arrays) // (1 << 20) + 4,
    )


def group_list(size):
    stages = stage_list(size)
    count = size // stages[0][1] - 1
    if len(stages) == 2 and count > 1:
        return [(0, 1), (1, count)]
    return [(0, count)]


def gather_rows(block, size):
    *far, (stride, radix) = stage_list(size)[::-1]
    rest = []
    for far_stride, far_radix in far:
        whole = join([block] + rest) if rest else block
        rest += [swap(whole, size, k * far_stride) for k in range(1, far_radix)]
    parts = {k: [swap(block, size, k * stride)] for k in range(radix - 1, 0, -1)}
    parts[0] = [block]
    if len(far) > 1:
        rest = [join(rest)]
    groups = group_list(size) if len(far) == 1 else [(0, 1)]
    for low, high in groups:
        piece = rest[low] if high - low == 1 else join(rest[low:high])
        parts[0].append(piece)
        for k in range(radix - 1, 0, -1):
            parts[k].append(swap(piece, size, k * stride))
    return [part for k in range(radix) for part in parts[k]]


def scatter_sum(pieces, size):
    (stride, radix), *far = stage_list(size)
    groups = group_list(size)
    rows = pieces[0][0].shape[0]
    order = range(radix - 1, 0, -1)
    back = {}
    for g in range(len(groups), 0, -1):
        for k in order:
            back[g, k] = swap(pieces[k][g], size, k * stride)
    side = {k: swap(pieces[k][0], size, k * stride) for k in order}
    terms = {
        g: [(pieces[0][g], 0)] + [(back[g, k], 0) for k in order]
        for g in range(1, len(groups) + 1)
    }
    last = [(pieces[0][0], 0)] + [(side[k], 0) for k in order]
    if len(far) == 1:
        far_stride = far[0][0]
        for g in range(len(groups), 0, -1):
            low, high = groups[g - 1]
            spans = [(i * rows, (i + 1) * rows, BF16) for i in range(high - low)]
            sends = fold(terms[g], spans)
            for i in range(high - low - 1, -1, -1):
                k = low + i + 1
                last.append((swap(sends[i], size, k * far_stride), 0))
    else:
        terms, count = terms[1], pieces[0][1].shape[0]
        for far_stride, far_radix in far:
            part = (count + rows) // far_radix
            spans = [(k * part - rows, (k + 1) * part - rows, BF16) for k in range(1, far_radix)]
            if part > rows:
                spans.append((0, part - rows, F32))
            sums = fold(terms, spans)
            moved = [swap(sums[k - 1], size, k * far_stride) for k in range(1, far_radix)]
            terms = [(sums[-1], 0)] + [(value, rows) for value in moved]
            last += [(value, 0) for value in moved]
            count = part - rows
    return fold(last, [(0, rows, BF16)])[0]


def split_kernel(*refs, chunk):
    count = (len(refs) - 1) // 3
    stored, outs, slots, sems = refs[:count], refs[count : 2 * count], refs[2 * count : -1], refs[-1]
    half = LANES
    row = lax.broadcasted_iota(jnp.int32, (2 * half, 2 * half), 0)
    column = lax.broadcasted_iota(jnp.int32, (2 * half, 2 * half), 1)
    order = (column == 2 * (row % half) + row // half).astype(F32).astype(BF16)
    work = []
    for i, stored_ref in enumerate(stored):
        for step in range(stored_ref.shape[0] // chunk):
            place = pl.ds(step * chunk, chunk)
            copy = pltpu.make_async_copy(stored_ref.at[place], slots[i].at[place], sems.at[len(work)])
            copy.start()
            work.append((copy, i, step))
    for copy, i, step in work:
        copy.wait()
        width = stored[i].shape[2]
        for part in range(chunk // half):
            rows = pl.ds(step * chunk + part * half, half)
            pairs = slots[i][rows].reshape(2 * half, width)
            apart = jnp.dot(order, pairs, preferred_element_type=F32).astype(BF16)
            outs[i][rows, :width] = apart[:half]
            outs[i][rows, width:] = apart[half:]


def split_pairs(*weights):
    chunk = 4 * LANES
    steps = sum(w.shape[0] // chunk for w in weights)
    return call(
        functools.partial(split_kernel, chunk=chunk),
        [like((w.shape[0], 2 * w.shape[2]), BF16) for w in weights],
        [HBM] * len(weights),
        tuple(pltpu.with_memory_space_constraint(w, pltpu.HBM) for w in weights),
        28,
        scratch=[pltpu.VMEM(w.shape, BF16) for w in weights] + [pltpu.SemaphoreType.DMA((steps,))],
        flops=sum(4 * 2 * LANES * w.size for w in weights),
    )


def gate_up_kernel(*refs, count, depth):
    parts, weight_ref, send_ref, own_ref = refs[:count], *refs[count : count + 3]
    rows = jnp.concatenate([part[:, :depth] for part in parts], axis=0)
    total = jnp.dot(rows, weight_ref[...], preferred_element_type=F32)
    own_ref[...] = total
    send_ref[...] = total.astype(BF16)
    for extra_ref in refs[count + 3 :]:
        extra_ref[...] = jnp.concatenate([part[:, depth:] for part in parts], axis=0)


def gate_up(parts, weight, extra=False):
    depth, width = weight.shape
    rows = sum(part.shape[0] for part in parts)
    outs = [like((rows, width), BF16), like((rows, width), F32)]
    if extra:
        outs.append(like((rows, LANES), BF16))
    return call(
        functools.partial(gate_up_kernel, count=len(parts), depth=depth),
        outs,
        [VMEM] * (len(parts) + 1),
        (*parts, weight),
        20 + rows * width // (1 << 17) * 2,
        flops=2 * rows * depth * width,
    )


def sub_swap(send):
    return lax.ppermute(send, "sub", [(0, 1), (1, 0)])


def hidden_of(own_ref, moved_ref, scale=None):
    total = own_ref[...] + moved_ref[...].astype(F32)
    if scale is not None:
        total = total * scale
    width = total.shape[1] // 2
    gate = total[:, :width]
    return (gate / (1.0 + jnp.exp(-gate)) * total[:, width:]).astype(BF16)


def shared_down_kernel(own_ref, moved_ref, weight_ref, out_ref):
    hidden = hidden_of(own_ref, moved_ref)
    out_ref[...] = jnp.dot(hidden, weight_ref[...], preferred_element_type=F32)


def piece_spans(rows, size):
    return [(0, rows)] + [((low + 1) * rows, (high + 1) * rows) for low, high in group_list(size)]


def routed_down_kernel(
    own_ref, moved_ref, extra_ref, base_ref, weight_ref, *outs, spans
):
    expert = (lax.axis_index("ep") // EXP_ROWS).astype(F32)
    extra = extra_ref[...].astype(F32)
    gate = extra[:, 1:2] + extra[:, 2:3]
    hidden = hidden_of(own_ref, moved_ref, jnp.where(extra[:, :1] == expert, gate, 0.0))
    partial = base_ref[...] + jnp.dot(hidden, weight_ref[...], preferred_element_type=F32)
    for out_ref, (low, high) in zip(outs, spans):
        out_ref[...] = partial[low:high].astype(out_ref.dtype)


def dense_experts(parts, shared_in, routed_in, shared_down, expert_down, rows, size):
    send_s, own_s, extra = gate_up(parts, shared_in, extra=True)
    moved_s = sub_swap(send_s)
    send_r, own_r = gate_up(parts, routed_in)
    moved_r = sub_swap(send_r)
    total_rows, width = send_s.shape[0], shared_down.shape[1]
    base = call(
        shared_down_kernel,
        like((total_rows, width), F32),
        [VMEM] * 3,
        (own_s, moved_s, shared_down),
        16,
        flops=2 * total_rows * shared_down.size,
    )
    radix = stage_list(size)[0][1]
    count = total_rows // radix
    inner = piece_spans(rows, size)
    spans = [(k * count + low, k * count + high) for k in range(radix) for low, high in inner]
    pieces = call(
        functools.partial(routed_down_kernel, spans=spans),
        [like((high - low, width), F32 if low < count else BF16) for low, high in spans],
        [VMEM] * 5,
        (own_r, moved_r, extra, base, expert_down),
        20,
        flops=2 * total_rows * expert_down.size,
    )
    step = len(inner)
    return scatter_sum([pieces[k * step : (k + 1) * step] for k in range(radix)], size)


def slot_experts(
    parts, shared_in, routed_in, shared_down, expert_down, rows, size, capacity, own_expert
):
    half_width = shared_in.shape[0]
    packed = jnp.concatenate(parts, axis=0)
    all_tokens = packed[:, :half_width]
    extra = packed[:, half_width:]
    all_gates = extra[:, 1].astype(F32) + extra[:, 2].astype(F32)
    picked = (extra[:, 0].astype(jnp.int32) == own_expert).reshape(size, rows).astype(jnp.int32)
    position = jnp.cumsum(picked, axis=1) - picked
    block = lax.broadcasted_iota(jnp.int32, (size, rows), 0)
    slot = jnp.where(picked == 1, block * capacity + position, -1).reshape(-1)
    slots = lax.broadcasted_iota(jnp.int32, (size * capacity, size * rows), 0)
    select = (slots == slot[None, :]).astype(BF16)
    weighted = (all_gates[:, None] * all_tokens.astype(F32)).astype(BF16)
    slot_rows = jnp.dot(select, weighted, preferred_element_type=F32).astype(BF16)

    def hidden(x, weight):
        total = jnp.dot(x, weight, preferred_element_type=F32)
        total = total + sub_swap(total.astype(BF16)).astype(F32)
        width = total.shape[1] // 2
        return (jax.nn.silu(total[:, :width]) * total[:, width:]).astype(BF16)

    shared = jnp.dot(hidden(all_tokens, shared_in), shared_down, preferred_element_type=F32)
    routed = jnp.dot(hidden(slot_rows, routed_in), expert_down, preferred_element_type=F32)
    partial = shared + lax.dot_general(
        select, routed.astype(BF16), (((0,), (0,)), ((), ())), preferred_element_type=F32
    )
    radix = stage_list(size)[0][1]
    count = partial.shape[0] // radix
    pieces = []
    for k in range(radix):
        block = partial[k * count : (k + 1) * count].astype(F32 if k == 0 else BF16)
        pieces.append([block[low:high] for low, high in piece_spans(rows, size)])
    return scatter_sum(pieces, size)


def local(
    tokens, expert_ids, router_score, expert_gate_up, expert_down, shared_gate_up, shared_down
):
    rows = tokens.shape[0]
    size = lax.axis_size("ep")
    experts = size // EXP_ROWS
    capacity = min(rows, max(2, 3 * rows // experts))

    parts = gather_rows(pack(tokens, expert_ids, router_score), size)
    shared_in, routed_in = split_pairs(shared_gate_up, expert_gate_up)
    operands = (parts, shared_in, routed_in, shared_down, expert_down, rows, size)
    if capacity == rows:
        mixed = dense_experts(*operands)
    else:
        mixed = slot_experts(*operands, capacity, lax.axis_index("ep") // EXP_ROWS)
    return mixed


def solution(mesh):
    placed = (
        P(("rep", "ep"), "sub"),
        P(("rep", "ep"), None),
        P(("rep", "ep"), None),
        P("sub", None, "ep"),
        P("ep", "sub"),
        P("sub", None, "ep"),
        P("ep", "sub"),
    )
    return jax.shard_map(
        local, mesh=mesh, in_specs=placed, out_specs=P(("rep", "ep"), "sub"), check_vma=False
    )
```

```python
import functools

import jax
import jax.numpy as jnp
from jax import lax
from jax.experimental import pallas as pl
from jax.experimental.pallas import tpu as pltpu
from jax.sharding import PartitionSpec as P


EXP_ROWS = 8
LANES = 128
F32 = jnp.float32
BF16 = jnp.bfloat16
VMEM = pl.BlockSpec(memory_space=pltpu.VMEM)
HBM = pl.BlockSpec(memory_space=pltpu.HBM)
GATHER_GROUPS = ((0, 2), (2, 4))
SCATTER_GROUPS = ((0, 1), (1, 2), (2, 4))


def stage_list(size):
    stages = []
    stride = 1
    while stride < size:
        radix = 4 if size // stride % 4 == 0 else 2
        stages.append((stride, radix))
        stride *= radix
    return stages


def swap(value, size, offset):
    return lax.ppermute(value, "ep", [(i, i ^ offset) for i in range(size)])


def call(body, outs, ins, args, limit, scratch=(), flops=0):
    return pl.pallas_call(
        body,
        out_shape=outs,
        in_specs=ins,
        out_specs=jax.tree.map(lambda _: VMEM, outs),
        scratch_shapes=scratch,
        compiler_params=pltpu.CompilerParams(vmem_limit_bytes=limit << 20),
        cost_estimate=pl.CostEstimate(
            flops=flops,
            bytes_accessed=sum(a.size * a.dtype.itemsize for a in args),
            transcendentals=0,
        ),
    )(*args)


def like(shape, dtype):
    return jax.ShapeDtypeStruct(shape, dtype)


def pack_kernel(tokens_hbm, ids_hbm, score_hbm, out_ref, ids_ref, score_ref, sems):
    rows, width = tokens_hbm.shape
    copies = [
        pltpu.make_async_copy(ids_hbm, ids_ref, sems.at[0]),
        pltpu.make_async_copy(score_hbm, score_ref, sems.at[1]),
        pltpu.make_async_copy(tokens_hbm, out_ref.at[:, pl.ds(0, width)], sems.at[2]),
    ]
    for copy in copies:
        copy.start()
    here = lax.broadcasted_iota(jnp.int32, (rows, rows), 0)
    there = lax.broadcasted_iota(jnp.int32, (rows, rows), 1)

    def column(row):
        return jnp.sum(jnp.where(here == there, row, 0.0), axis=1, keepdims=True)

    copies[0].wait()
    copies[1].wait()
    ids = column(ids_ref[...].astype(F32))
    gate = 1.0 / (1.0 + jnp.exp(-column(score_ref[...])))
    high = gate.astype(BF16).astype(F32)
    lane = lax.broadcasted_iota(jnp.int32, (rows, LANES), 1)
    extra = jnp.where(lane == 0, ids, jnp.where(lane == 1, high, gate - high))
    out_ref[:, width:] = extra.astype(BF16)
    copies[2].wait()


def pack(tokens, ids, score):
    rows, width = tokens.shape
    arrays = (tokens, ids.reshape(1, rows), score.reshape(1, rows))
    return call(
        pack_kernel,
        like((rows, width + LANES), BF16),
        [HBM] * 3,
        tuple(pltpu.with_memory_space_constraint(a, pltpu.HBM) for a in arrays),
        2,
        scratch=[
            pltpu.VMEM((1, rows), jnp.int32),
            pltpu.VMEM((1, rows), F32),
            pltpu.SemaphoreType.DMA((3,)),
        ],
    )


def join_kernel(*refs):
    *parts, out_ref = refs
    row = 0
    for part in parts:
        out_ref[row : row + part.shape[0]] = part[...]
        row += part.shape[0]


def join(parts):
    rows = sum(part.shape[0] for part in parts)
    return call(
        join_kernel, like((rows, parts[0].shape[1]), BF16), [VMEM] * len(parts), tuple(parts), 8
    )


def fold_kernel(*refs, sums):
    outs = refs[len(refs) - len(sums) :]
    for out_ref, terms in zip(outs, sums):
        rows = out_ref.shape[0]
        total = None
        for index, offset in terms:
            value = refs[index][offset : offset + rows].astype(F32)
            total = value if total is None else total + value
        out_ref[...] = total.astype(out_ref.dtype)


def fold(sums):
    arrays = []
    for terms, _, _ in sums:
        arrays += [array for array, _ in terms if not any(array is other for other in arrays)]
    place = {id(array): index for index, array in enumerate(arrays)}
    return call(
        functools.partial(
            fold_kernel,
            sums=tuple(
                tuple((place[id(array)], offset) for array, offset in terms) for terms, _, _ in sums
            ),
        ),
        [like((rows, arrays[0].shape[1]), kind) for _, rows, kind in sums],
        [VMEM] * len(arrays),
        tuple(arrays),
        sum(a.size * a.dtype.itemsize for a in arrays) // (1 << 20) + 4,
    )


def plan(size, groups):
    (_, radix), *far = stage_list(size)
    if len(far) == 1 and far[0][1] == 4:
        return groups
    return (0, 1), (1, size // radix)


def gather_rows(block, size):
    *far, (stride, radix) = stage_list(size)[::-1]
    held = [block]
    for far_stride, far_radix in far:
        whole = join(held) if len(held) > 1 else block
        held += [swap(whole, size, k * far_stride) for k in range(1, far_radix)]
    groups = plan(size, GATHER_GROUPS)
    if len(far) != 1:
        held, groups = [block, join(held[1:])], ((0, 1), (1, 2))
    parts = [[] for _ in range(radix)]
    for low, high in groups:
        piece = held[low] if high - low == 1 else join(held[low:high])
        parts[0].append(piece)
        for k in range(radix - 1, 0, -1):
            parts[k].append(swap(piece, size, k * stride))
    return [part for k in range(radix) for part in parts[k]]


def scatter_spans(rows, size):
    return [(low * rows, high * rows) for low, high in plan(size, SCATTER_GROUPS)]


def scatter_sum(pieces, size):
    (stride, radix), *far = stage_list(size)
    groups = plan(size, SCATTER_GROUPS)
    rows = pieces[0][0].shape[0] // (groups[0][1] - groups[0][0])
    back = {}
    for g in range(len(groups) - 1, -1, -1):
        for k in range(radix - 1, 0, -1):
            back[g, k] = swap(pieces[k][g], size, k * stride)

    def terms_of(index):
        (g,) = [g for g, (low, high) in enumerate(groups) if low <= index < high]
        offset = (index - groups[g][0]) * rows
        found = [(pieces[0][g], offset)]
        return found + [(back[g, k], offset) for k in range(radix - 1, 0, -1)]

    ends = terms_of(0)
    if len(far) == 1:
        for low, high in groups[::-1]:
            if high == 1:
                continue
            indices = range(high - 1, max(low, 1) - 1, -1)
            sends = fold([(terms_of(i), rows, BF16) for i in indices])
            for i, send in zip(indices, sends):
                ends.append((swap(send, size, i * far[0][0]), 0))
    else:
        terms, count = terms_of(1), pieces[0][1].shape[0]
        for far_stride, far_radix in far:
            part = (count + rows) // far_radix

            def shifted(low):
                return [(array, offset + low) for array, offset in terms]

            sums = [(shifted(k * part - rows), part, BF16) for k in range(1, far_radix)]
            if part > rows:
                sums.append((shifted(0), part - rows, F32))
            sends = fold(sums)
            moved = [swap(sends[k - 1], size, k * far_stride) for k in range(1, far_radix)]
            terms = [(sends[-1], 0)] + [(value, rows) for value in moved]
            ends += [(value, 0) for value in moved]
            count = part - rows
    return fold([(ends, rows, BF16)])[0]


def split_kernel(*refs, chunk):
    count = (len(refs) - 1) // 3
    stored, outs, slots, sems = refs[:count], refs[count : 2 * count], refs[2 * count : -1], refs[-1]
    half = LANES
    row = lax.broadcasted_iota(jnp.int32, (2 * half, 2 * half), 0)
    column = lax.broadcasted_iota(jnp.int32, (2 * half, 2 * half), 1)
    order = (column == 2 * (row % half) + row // half).astype(F32).astype(BF16)
    work = []
    for i, stored_ref in enumerate(stored):
        for step in range(stored_ref.shape[0] // chunk):
            place = pl.ds(step * chunk, chunk)
            copy = pltpu.make_async_copy(stored_ref.at[place], slots[i].at[place], sems.at[len(work)])
            copy.start()
            work.append((copy, i, step))
    for copy, i, step in work:
        copy.wait()
        width = stored[i].shape[2]
        for part in range(chunk // half):
            rows = pl.ds(step * chunk + part * half, half)
            pairs = slots[i][rows].reshape(2 * half, width)
            apart = jnp.dot(order, pairs, preferred_element_type=F32).astype(BF16)
            outs[i][rows, :width] = apart[:half]
            outs[i][rows, width:] = apart[half:]


def split_pairs(*weights):
    chunk = 2 * LANES
    steps = sum(w.shape[0] // chunk for w in weights)
    return call(
        functools.partial(split_kernel, chunk=chunk),
        [like((w.shape[0], 2 * w.shape[2]), BF16) for w in weights],
        [HBM] * len(weights),
        tuple(pltpu.with_memory_space_constraint(w, pltpu.HBM) for w in weights),
        4 + sum(w.size for w in weights) * 5 >> 20,
        scratch=[pltpu.VMEM(w.shape, BF16) for w in weights] + [pltpu.SemaphoreType.DMA((steps,))],
        flops=sum(4 * 2 * LANES * w.size for w in weights),
    )


def gate_up_kernel(*refs, starts, held_starts, depth):
    count = len(starts)
    parts, weight_ref, refs = refs[:count], refs[count], refs[count + 1 :]
    held = refs[: len(refs) // 2] if held_starts else ()
    outs = refs[len(held) :]
    rows = jnp.concatenate([part[:, :depth] for part in parts], axis=0)
    total = jnp.dot(rows, weight_ref[...], preferred_element_type=F32)
    extra = jnp.concatenate([part[:, depth:] for part in parts], axis=0)
    for out_ref, value in zip(outs, (total.astype(BF16), total, extra)):
        low = 0
        for part, start in zip(parts, starts):
            out_ref[start : start + part.shape[0]] = value[low : low + part.shape[0]]
            low += part.shape[0]
    for held_ref, out_ref in zip(held, outs):
        for low, start, length in held_starts:
            out_ref[start : start + length] = held_ref[low : low + length]


def gate_up(parts, starts, weight, extra, held=(), held_starts=()):
    depth, width = weight.shape
    rows = sum(part.shape[0] for part in parts)
    full = rows + sum(length for _, _, length in held_starts)
    outs = [like((full, width), BF16), like((full, width), F32)]
    if extra:
        outs.append(like((full, LANES), BF16))
    return call(
        functools.partial(gate_up_kernel, starts=starts, held_starts=held_starts, depth=depth),
        outs,
        [VMEM] * (len(parts) + 1 + len(held)),
        (*parts, weight, *held),
        24,
        flops=2 * rows * depth * width,
    )


def gate_up_twice(parts, late, weight, extra=False):
    starts = [sum(part.shape[0] for part in parts[:i]) for i in range(len(parts))]
    early = [i for i in range(len(parts)) if i not in late]
    first, low = [], 0
    for i in early:
        first.append((low, starts[i], parts[i].shape[0]))
        low += parts[i].shape[0]
    held = gate_up([parts[i] for i in early], tuple(low for low, _, _ in first), weight, extra)
    return gate_up(
        [parts[i] for i in late],
        tuple(starts[i] for i in late),
        weight,
        extra,
        tuple(held),
        tuple(first),
    )


def sub_swap(send):
    return lax.ppermute(send, "sub", [(0, 1), (1, 0)])


def hidden_of(own, moved, scale=None):
    total = own + moved.astype(F32)
    if scale is not None:
        total = total * scale
    width = total.shape[1] // 2
    gate = total[:, :width]
    return (gate / (1.0 + jnp.exp(-gate)) * total[:, width:]).astype(BF16)


def shared_down_kernel(own_ref, moved_ref, weight_ref, out_ref):
    hidden = hidden_of(own_ref[...], moved_ref[...])
    out_ref[...] = jnp.dot(hidden, weight_ref[...], preferred_element_type=F32)


def routed_down_kernel(own_ref, moved_ref, extra_ref, base_ref, weight_ref, *outs, spans):
    def rows_of(ref):
        return jnp.concatenate([ref[low:high] for low, high in spans], axis=0)

    expert = (lax.axis_index("ep") // EXP_ROWS).astype(F32)
    extra = rows_of(extra_ref).astype(F32)
    gate = extra[:, 1:2] + extra[:, 2:3]
    scale = jnp.where(extra[:, :1] == expert, gate, 0.0)
    hidden = hidden_of(rows_of(own_ref), rows_of(moved_ref), scale)
    partial = jnp.dot(hidden, weight_ref[...], preferred_element_type=F32)
    row = 0
    for out_ref, (low, high) in zip(outs, spans):
        total = partial[row : row + high - low] + base_ref[low:high]
        out_ref[...] = total.astype(out_ref.dtype)
        row += high - low


def dense_experts(parts, shared_in, routed_in, shared_down, expert_down, rows, size):
    radix = stage_list(size)[0][1]
    step = len(parts) // radix
    late = [k * step + step - 1 for k in range(1, radix)]
    send_s, own_s, extra = gate_up_twice(parts, late, shared_in, extra=True)
    moved_s = sub_swap(send_s)
    send_r, own_r = gate_up_twice(parts, late, routed_in)
    moved_r = sub_swap(send_r)
    total_rows, width = send_s.shape[0], shared_down.shape[1]
    base = call(
        shared_down_kernel,
        like((total_rows, width), F32),
        [VMEM] * 3,
        (own_s, moved_s, shared_down),
        16,
        flops=2 * total_rows * shared_down.size,
    )
    count = total_rows // radix
    inner = scatter_spans(rows, size)
    pieces = [[None] * len(inner) for _ in range(radix)]

    def down_routed(chosen):
        spans = [(k * count + inner[g][0], k * count + inner[g][1]) for k, g in chosen]
        outs = call(
            functools.partial(routed_down_kernel, spans=spans),
            [like((high - low, width), F32 if low < count else BF16) for low, high in spans],
            [VMEM] * 5,
            (own_r, moved_r, extra, base, expert_down),
            20,
            flops=2 * sum(high - low for low, high in spans) * expert_down.size,
        )
        for (k, g), out in zip(chosen, outs):
            pieces[k][g] = out

    final = len(inner) - 1
    down_routed([(k, final) for k in range(radix)])
    down_routed([(k, g) for k in range(radix) for g in range(final)])
    return scatter_sum(pieces, size)


def slot_experts(
    parts, shared_in, routed_in, shared_down, expert_down, rows, size, capacity, own_expert
):
    half_width = shared_in.shape[0]
    packed = jnp.concatenate(parts, axis=0)
    all_tokens = packed[:, :half_width]
    extra = packed[:, half_width:]
    all_gates = extra[:, 1].astype(F32) + extra[:, 2].astype(F32)
    picked = (extra[:, 0].astype(jnp.int32) == own_expert).reshape(size, rows).astype(jnp.int32)
    position = jnp.cumsum(picked, axis=1) - picked
    block = lax.broadcasted_iota(jnp.int32, (size, rows), 0)
    slot = jnp.where(picked == 1, block * capacity + position, -1).reshape(-1)
    slots = lax.broadcasted_iota(jnp.int32, (size * capacity, size * rows), 0)
    select = (slots == slot[None, :]).astype(BF16)
    weighted = (all_gates[:, None] * all_tokens.astype(F32)).astype(BF16)
    slot_rows = jnp.dot(select, weighted, preferred_element_type=F32).astype(BF16)

    def hidden(x, weight):
        total = jnp.dot(x, weight, preferred_element_type=F32)
        total = total + sub_swap(total.astype(BF16)).astype(F32)
        width = total.shape[1] // 2
        return (jax.nn.silu(total[:, :width]) * total[:, width:]).astype(BF16)

    shared = jnp.dot(hidden(all_tokens, shared_in), shared_down, preferred_element_type=F32)
    routed = jnp.dot(hidden(slot_rows, routed_in), expert_down, preferred_element_type=F32)
    partial = shared + lax.dot_general(
        select, routed.astype(BF16), (((0,), (0,)), ((), ())), preferred_element_type=F32
    )
    radix = stage_list(size)[0][1]
    count = partial.shape[0] // radix
    pieces = []
    for k in range(radix):
        block = partial[k * count : (k + 1) * count].astype(F32 if k == 0 else BF16)
        pieces.append([block[low:high] for low, high in scatter_spans(rows, size)])
    return scatter_sum(pieces, size)


def local(
    tokens, expert_ids, router_score, expert_gate_up, expert_down, shared_gate_up, shared_down
):
    rows = tokens.shape[0]
    size = lax.axis_size("ep")
    experts = size // EXP_ROWS
    capacity = min(rows, max(2, 3 * rows // experts))

    parts = gather_rows(pack(tokens, expert_ids, router_score), size)
    (shared_in,) = split_pairs(shared_gate_up)
    (routed_in,) = split_pairs(expert_gate_up)
    operands = (parts, shared_in, routed_in, shared_down, expert_down, rows, size)
    if capacity == rows:
        mixed = dense_experts(*operands)
    else:
        mixed = slot_experts(*operands, capacity, lax.axis_index("ep") // EXP_ROWS)
    return mixed


def solution(mesh):
    placed = (
        P(("rep", "ep"), "sub"),
        P(("rep", "ep"), None),
        P(("rep", "ep"), None),
        P("sub", None, "ep"),
        P("ep", "sub"),
        P("sub", None, "ep"),
        P("ep", "sub"),
    )
    return jax.shard_map(
        local, mesh=mesh, in_specs=placed, out_specs=P(("rep", "ep"), "sub"), check_vma=False
    )
```
